32 devices in a mesh: ckpt: 2 (over y), row: 4 (over z), col: 4 (over x, core).
Axes of the slice: x: 2, y: 2, z: 4, core: 2. Of those that a mesh axis runs over, the one named last changes fastest.
Arguments:
- grad_slab: bfloat16 [768, 27648], P(('ckpt', 'col'), 'row'), parts along dimension 0, may hold values from -6 to 6
- eigenbasis: bfloat16 [55296, 14336], P(('ckpt', 'row'), 'col'), parts along dimension 0, may hold values from -0.0546875 to 0.0546875
- eigenvalues: bfloat16 [768, 14336], P('ckpt', 'col'), parts along dimension 0, may hold values from 0.049804688 to 5
Outputs:
- preconditioned: bfloat16 [768, 27648], P(('ckpt', 'col'), 'row'), parts along dimension 0
The draws below stay inside these ranges and needn't reach their ends.
There are 2 independent parts, one for each index of `ckpt`. The reference program is written for one: setup_inputs(seed, part) draws one part's arguments, and reference() takes and returns one part's arrays. A program takes and returns all parts, laid end to end along the dimension named above; each array names one. Nothing has to cross between parts.
All inputs are finite; a program needn't handle non-finite values.
Results may differ from the reference program's by a relative error of at most 0.0046.
Values may be sent and summed in bfloat16 or wider, within the bound.
No kernel may reach another device: no remote copies, remote signals or barrier semaphores. Data moves between devices by JAX's collectives and lax.ppermute only.
A program may use at most 128 MiB of HBM per device.

```python
import math
import jax
import jax.numpy as jnp
from jax import lax

FF = 27648
EIGW = 14336
S = 384


def raised(entries, key, source, target, shards_of, factor):
    owner, partner = [(jnp.arange(entries.shape[dim]) // (entries.shape[dim] // shards_of)).reshape([-1 if axis == dim else 1 for axis in range(entries.ndim)]) for dim in (source, target)]
    chosen = jax.random.permutation(key, shards_of)[partner]
    strong = (owner == chosen) | (owner == (partner + shards_of // 2) % shards_of)
    return jnp.where(strong, factor * entries, entries)


def levels(stream_key, extent, shards, low, top_value):
    level = 1.0
    for dim, parts in shards:
        heights = jax.random.uniform(jax.random.fold_in(jax.random.fold_in(stream_key, 6), dim), (parts,), jnp.float32, low / len(shards), top_value / len(shards))
        level = level * jnp.repeat(jnp.exp(heights), extent[dim] // parts).reshape((-1,) + (1,) * (len(extent) - 1 - dim))
    return level


def noise(stream_key, shape, spread, limit, pieces=(), kind=jnp.bfloat16):
    level = levels(stream_key, shape, pieces, -0.22, 0.18) if pieces else 1.0
    values = jax.random.normal(stream_key, shape, jnp.float32) * spread * level
    return jnp.minimum(jnp.maximum(values, -limit), limit).astype(kind)


def bell_draw_with(stream_key, shape, scale, most, pieces, heavy, kind=jnp.bfloat16):
    values = scale * jax.random.normal(stream_key, shape, jnp.float32)
    if pieces:
        values = values * levels(stream_key, shape, pieces, -0.22, 0.18)
    return jnp.clip(raised(values, jax.random.fold_in(stream_key, 3), *heavy), -most, most).astype(kind)


def setup_inputs(seed: int = 0, part: int = 0) -> dict:
    splits = jax.random.split(jax.random.key(seed), 4)
    own_keys = jax.random.split(jax.random.fold_in(splits[3], part), 4)
    return {
        "grad_slab": noise(own_keys[0], (S, FF), 1.0, 6.0, ((0, 4), (1, 4))),
        "eigenbasis": bell_draw_with(own_keys[1], (FF, EIGW), FF ** -0.5, 0.0546875, ((0, 4), (1, 4)), (0, 1, 4, 2.0)),
        "eigenvalues": jnp.clip(jnp.exp(math.log(5.0) - 4.609084 * jax.random.uniform(own_keys[2], (S, EIGW), jnp.float32) ** levels(own_keys[2], (S, EIGW), ((1, 4),), -0.2, 0.2)), 0.049804688, 5.0).astype(jnp.bfloat16),
    }


DAMPING = 0.1


def reference(grad_slab, eigenbasis, eigenvalues):
    rotated = jnp.dot(grad_slab, eigenbasis, preferred_element_type=jnp.float32)
    scaled = (rotated / (eigenvalues.astype(jnp.float32) + DAMPING)).astype(jnp.bfloat16)
    result = lax.dot_general(scaled, eigenbasis, (((1,), (1,)), ((), ())), preferred_element_type=jnp.float32)
    return result.astype(jnp.bfloat16)
```

```python
import functools

import jax
import jax.numpy as jnp
from jax import lax
from jax.experimental import pallas as pl
from jax.experimental.pallas import tpu as pltpu
from jax.sharding import PartitionSpec as P

DAMPING = 0.1
AHEAD = 2
PARTS = 3
MIB = 1 << 20
F32, BF16 = jnp.float32, jnp.bfloat16
ANY = pl.BlockSpec(memory_space=pl.ANY)
SMEM = pl.BlockSpec(memory_space=pltpu.SMEM)


class Chain:
    last = ()


def shape(dims, dtype):
    return jax.ShapeDtypeStruct(dims, dtype)


def whole(a):
    return pl.BlockSpec(a.shape, lambda j: (0,) * len(a.shape))


def tile_of(extent, most=256):
    return next(t for t in range(most, 0, -128) if extent % t == 0)


def chained(kernel, at, more, outs, *refs):
    refs[at + more + outs][...] = jnp.zeros((8, 128), F32)
    kernel(*refs[:at], *refs[at + more : at + more + outs], *refs[at + more + outs + 1 :])


def call(chain, kernel, steps, outs, in_specs, out_specs, args, flops, moved, scratch=(), vmem=8):
    token = shape((8, 128), F32)
    result = pl.pallas_call(
        functools.partial(chained, kernel, len(args), len(chain.last), len(outs)),
        grid=(steps,),
        out_shape=(*outs, token),
        in_specs=[*in_specs] + [ANY] * len(chain.last),
        out_specs=(*out_specs, whole(token)),
        scratch_shapes=list(scratch),
        compiler_params=pltpu.CompilerParams(vmem_limit_bytes=vmem * MIB),
        cost_estimate=pl.CostEstimate(flops=flops, bytes_accessed=moved, transcendentals=0),
    )(*args, *chain.last)
    chain.last = (result[-1],)
    return result[:-1]


def dot_kernel(n, *refs):
    xs, (e, pb, held) = refs[:n], refs[n:]
    j, depth = pl.program_id(0), e.shape[0]
    cols = pl.ds(pl.multiple_of(j * depth, 128), depth)
    part = jnp.dot(jnp.concatenate([x[:, cols] for x in xs], 0), e[...], preferred_element_type=F32)

    @pl.when(j == 0)
    def _():
        held[...] = part

    @pl.when(j > 0)
    def _():
        held[...] += part

    @pl.when(j == pl.num_programs(0) - 1)
    def _():
        pb[...] = held[...].astype(BF16)


def dot(chain, xs, e, width, k):
    rows, depth = sum(x.shape[0] for x in xs), e.shape[0]
    deep = tile_of(depth, 768)
    return call(
        chain,
        functools.partial(dot_kernel, len(xs)),
        depth // deep,
        [shape((rows, width), BF16)],
        [whole(x) for x in xs] + [pl.BlockSpec((deep, width), lambda j: (j, k))],
        [pl.BlockSpec((rows, width), lambda j: (0, 0))],
        (*xs, e),
        2 * rows * depth * width,
        depth * width * 2,
        [pltpu.VMEM((rows, width), F32)],
        vmem=24,
    )[0]


def columns(a, tile):
    return pl.BlockSpec((a.shape[0], tile), lambda j: (0, j))


def add_kernel(p, r, s, sb):
    total = p[...].astype(F32) + r[...].astype(F32)
    s[...] = total
    sb[...] = total.astype(BF16)


def add(chain, p, r):
    return call(
        chain,
        add_kernel,
        1,
        [shape(p.shape, F32), shape(p.shape, BF16)],
        [whole(p)] * 2,
        [whole(p)] * 2,
        (p, r),
        p.size,
        p.size * 10,
    )


def scale_kernel(n, s, r, *refs):
    o, at = refs[n], 0
    for values in refs[:n]:
        rows = slice(at, at + values.shape[0])
        total = s[rows, :] + r[rows, :].astype(F32)
        o[rows, :] = (total / (values[...].astype(F32) + DAMPING)).astype(BF16)
        at += values.shape[0]


def scale(chain, s, r, values, tile, first):
    return call(
        chain,
        functools.partial(scale_kernel, len(values)),
        s.shape[1] // tile,
        [shape(s.shape, BF16)],
        [columns(s, tile)] * 2
        + [pl.BlockSpec((v.shape[0], tile), lambda j: (0, first + j)) for v in values],
        [columns(s, tile)],
        (s, r, *values),
        s.size,
        s.size * 10,
    )[0]


def back(chain, chosen, e, start, first, last, before):
    chosen, chain.last = lax.optimization_barrier((chosen, chain.last))
    part = lax.dot_general(
        chosen,
        e[first:last, start : start + chosen.shape[1]],
        (((1,), (1,)), ((), ())),
        preferred_element_type=F32,
    )
    if before is not None:
        part += before
    part, chain.last = lax.optimization_barrier((part, chain.last))
    return part


def pair_kernel(p, r, o):
    o[...] = (p[...] + r[...].astype(F32)).astype(BF16)


def pair(chain, part, received):
    rows, features = received.shape[0] // 2, part.shape[1]
    tile = tile_of(features, 1152)
    block = pl.BlockSpec((rows, tile), lambda j: (1, j))
    return call(
        chain,
        pair_kernel,
        features // tile,
        [shape((rows, features), BF16)],
        [block] * 2,
        [pl.BlockSpec((rows, tile), lambda j: (0, j))],
        (part, received),
        2 * rows * features,
        8 * rows * features,
    )[0]


def final_kernel(steps, *refs):
    j = pl.program_id(0)
    for i in range(len(refs) // 3):
        own, other, crossed = refs[3 * i : 3 * i + 3]

        @pl.when(j // steps == i)
        def _():
            refs[-1][...] = (own[...] + other[...].astype(F32) + crossed[...].astype(F32)).astype(BF16)


def final(chain, triples):
    rows, features = triples[0][2].shape
    tile = tile_of(features, 1152)
    steps = features // tile
    block = lambda i: pl.BlockSpec((rows, tile), lambda j: (0, jnp.clip(j - i * steps, 0, steps - 1)))
    count = len(triples)
    return call(
        chain,
        functools.partial(final_kernel, steps),
        steps * count,
        [shape((rows, features * count), BF16)],
        [block(i) for i in range(count) for _ in range(3)],
        [pl.BlockSpec((rows, tile), lambda j: (0, j))],
        [a for triple in triples for a in triple],
        2 * rows * features * count,
        8 * rows * features * count,
    )[0]


def fast(grad, e, values):
    return preconditioned(grad, e, values)


def preconditioned(grad, e, values):
    chain = Chain()
    rows = grad.shape[0]
    tile = tile_of(e.shape[1])
    n = 2
    width, features = e.shape[1] // n, e.shape[0]
    me, z = lax.axis_index("col"), lax.axis_index("row")
    is_end = (z == 0) | (z == 3)

    def under(f, *args):
        return f(chain, *args)

    mate = lambda a: lax.ppermute(a, "col", [(0, 1), (1, 0), (2, 3), (3, 2)])
    across = lambda a: lax.ppermute(a, "col", [(0, 2), (2, 0), (1, 3), (3, 1)])
    inward = lambda a: lax.ppermute(a, "row", [(0, 1), (3, 2)])
    middle = lambda a: lax.ppermute(a, "row", [(1, 2), (2, 1)])
    outward = lambda a: lax.ppermute(a, "row", [(1, 0), (2, 3)])

    own_values = [lax.dynamic_slice_in_dim(values, (me ^ i) * rows, rows, 0) for i in range(4)]
    mate_rows = mate(grad)
    far = across(grad)
    units = [(g, k) for g in range(2) for k in range(n)]
    rotated, summed, mine, theirs = [], [], [], []

    def rotate(i):
        g, k = units[i]
        rotated.append(under(dot, sources[g], e, width, k))

    sources = [[grad, mate_rows]]
    for i in range(AHEAD):
        rotate(i)
    far, chain.last = lax.optimization_barrier((far, chain.last))
    sources.append([far, mate(far)])
    for i in range(len(units) + 2):
        if i < len(units):
            summed.append(under(add, rotated[i], inward(rotated[i])))
        if i + AHEAD < len(units):
            rotate(i + AHEAD)
        if 1 <= i <= len(units):
            (g, k), (s, sb) = units[i - 1], summed[i - 1]
            scaled = under(scale, s, middle(sb), own_values[2 * g : 2 * g + 2], tile, k * (width // tile))
            mine.append(scaled)
            theirs.append(outward(scaled))

    def rows_of(k):
        chosen = [jnp.where(is_end, theirs[g * n + k], mine[g * n + k]) for g in range(2)]
        return jnp.concatenate([c[p] for p in (slice(0, rows), slice(rows, None)) for c in chosen], 0)

    count = PARTS if features % (PARTS * 128) == 0 else 1
    size = features // count
    held = [None] * count
    for k in range(n - 1):
        chosen = rows_of(k)
        for h in range(count):
            held[h] = under(back, chosen, e, k * width, h * size, (h + 1) * size, held[h])
    chosen = rows_of(n - 1)
    received, crossed = [], []

    def cross(h):
        crossed.append(across(under(pair, held[h], received[h])))

    for h in range(count):
        held[h] = under(back, chosen, e, (n - 1) * width, h * size, (h + 1) * size, held[h])
        received.append(mate(held[h][2 * rows :].astype(BF16)))
        if h > 0:
            cross(h - 1)
    cross(count - 1)
    return final(chain, list(zip(held, received, crossed)))


def general(grad_slab, eigenbasis, eigenvalues):
    rotated_part = jnp.dot(
        lax.all_gather(grad_slab, "col", axis=0, tiled=True), eigenbasis, preferred_element_type=F32
    )
    own_share = lax.psum_scatter(rotated_part, "row", scatter_dimension=1, tiled=True)
    share_width = own_share.shape[1]
    offset = lax.axis_index("row") * share_width
    own_values = lax.dynamic_slice_in_dim(eigenvalues, offset, share_width, 1)
    scaled_share = (own_share / (own_values.astype(F32) + DAMPING)).astype(BF16)
    scaled = lax.all_gather(scaled_share, "row", axis=1, tiled=True)
    result = lax.psum_scatter(
        lax.dot_general(scaled, eigenbasis, (((1,), (1,)), ((), ())), preferred_element_type=F32),
        "col",
        scatter_dimension=0,
        tiled=True,
    )
    return result.astype(BF16)


def solution(mesh):
    placed = (P(("ckpt", "col"), "row"), P(("ckpt", "row"), "col"), P("ckpt", "col"))
    is_fast = mesh.shape["row"] == 4 and mesh.shape["col"] == 4
    return jax.shard_map(
        fast if is_fast else general,
        mesh=mesh,
        in_specs=placed,
        out_specs=P(("ckpt", "col"), "row"),
        check_vma=False,
    )
```
